256 devices in a mesh: dp: 8 (over z), pipe: 4 (over x), tensor: 8 (over y, core).
Axes of the slice: x: 4, y: 4, z: 8, core: 2. Of those that a mesh axis runs over, the one named last changes fastest.
Arguments:
- embeds: bfloat16 [32, 64, 4096], P('dp', 'tensor'), parts along dimension 0, may hold values from -6 to 6
- labels: int32 [32, 64], P('dp'), parts along dimension 0, may hold values from 0 to 24575
- norm_gain: float32 [4, 4096], P('pipe'), may hold values from 0.5 to 1.5
- w_query: bfloat16 [4, 4096, 2048], P('pipe', None, 'tensor'), may hold values from -0.09375 to 0.09375
- w_key: bfloat16 [4, 4096, 1024], P('pipe', None, 'tensor'), may hold values from -0.09375 to 0.09375
- w_value: bfloat16 [4, 4096, 1024], P('pipe', None, 'tensor'), may hold values from -0.09375 to 0.09375
- w_out: bfloat16 [4, 2048, 4096], P('pipe', 'tensor'), may hold values from -0.125 to 0.125
- final_gain: float32 [4096], replicated, may hold values from 0.5 to 1.5
- head_weight: bfloat16 [4096, 24576], P(None, ('pipe', 'tensor')), may hold values from -16 to 16
Outputs:
- token_loss: float32 [32, 64], P('dp', ('pipe', 'tensor')), parts along dimension 0
- scores: float32 [32], P('dp'), parts along dimension 0
The draws below stay inside these ranges and needn't reach their ends.
There are 8 independent parts, one for each index of `dp`. The reference program is written for one: setup_inputs(seed, part) draws one part's arguments, and reference() takes and returns one part's arrays. A program takes and returns all parts, laid end to end along the dimension named above; an argument that names none is the same for every part. Nothing has to cross between parts.
All inputs are finite; a program needn't handle non-finite values.
Results may differ from the reference program's by a relative error of at most 0.014.
Values may be sent and summed in bfloat16 or wider, within the bound.
No kernel may reach another device: no remote copies, remote signals or barrier semaphores. Data moves between devices by JAX's collectives and lax.ppermute only.
A program may use at most 64 MiB of HBM per device.

```python
import math
import jax
import jax.numpy as jnp
import numpy as np
from jax import lax

D = 4096
HD = 128
KVH = 8
QH = 16
MICRO = 4
SEQ = 64
LAYERS = 4
VOCAB = 24576
N_TENSOR = 8


def draw_head_weight(key, part):
    key_base, key_scale = jax.random.split(jax.random.fold_in(key, 17))
    base = jax.random.truncated_normal(key_base, -3.0, 3.0, (D, VOCAB), jnp.float32)
    column_scale = 3.0 + 0.0 * jax.random.uniform(key_scale, (1, VOCAB), jnp.float32)
    return (base * column_scale / math.sqrt(D)).astype(jnp.bfloat16)


def touch_ends(values, rng, smallest, top_value):
    extent = values.shape
    spot = [jax.random.randint(jax.random.fold_in(rng, axis), (), 0, extent[axis]) for axis in range(len(extent))]
    values = values.at[tuple(spot)].set(smallest)
    longest = extent.index(max(extent))
    spot[longest] = (spot[longest] + 1) % extent[longest]
    return values.at[tuple(spot)].set(top_value)


def level_of(own_key, dims, cuts, smallest, high):
    factor_of, own = 1.0, jax.random.fold_in(own_key, 6)
    for position, parts in cuts:
        heights = jnp.exp(jax.random.uniform(jax.random.fold_in(own, position), (parts,), jnp.float32, smallest / len(cuts), high / len(cuts)))
        factor_of = factor_of * jnp.repeat(heights, dims[position] // parts).reshape([-1 if axis == position else 1 for axis in range(len(dims))])
    return factor_of


def rank_table(number_of, slope):
    weights = [(1 << 20) // math.isqrt(standing ** slope) + 1 for standing in range(1, number_of + 1)]
    width = 1 + sum(weights) // (1 << 30)
    return np.cumsum(np.array([max(1, weight // width) for weight in weights]))


def ranked(own_key, shape, number_of, slope):
    listing = rank_table(number_of, slope)
    ticket = jax.random.randint(jax.random.fold_in(own_key, 1), shape, 0, int(listing[number_of - 1]))
    standing = jnp.searchsorted(jnp.asarray(listing, jnp.int32), ticket, side="right")
    return jax.random.permutation(jax.random.fold_in(own_key, 2), number_of)[standing].astype(jnp.int32)


def bell_draw(rng, dims, deviation, bound, cuts=(), kind=jnp.bfloat16):
    entries = jax.random.normal(rng, dims, jnp.float32) * deviation
    if len(cuts) > 0:
        entries = level_of(rng, dims, cuts, -0.22, 0.18) * entries
    return jnp.clip(entries, min=-bound, max=bound).astype(kind)


def setup_inputs(seed: int = 0, part: int = 0) -> dict:
    streams_of = jax.random.split(jax.random.key(seed), 10)
    part_splits = jax.random.split(jax.random.fold_in(streams_of[9], part), 10)
    return {
        "embeds": bell_draw(part_splits[0], (MICRO, SEQ, D), 1.0, 6.0, ((1, 8),)),
        "labels": touch_ends(ranked(part_splits[1], (MICRO, SEQ), VOCAB, 1), jax.random.fold_in(part_splits[1], 3), 0, VOCAB - 1).astype(jnp.int32),
        "norm_gain": jnp.clip(1.0 + 0.1 * jax.random.normal(streams_of[2], (LAYERS, D), jnp.float32), 0.5, 1.5),
        "w_query": bell_draw(streams_of[3], (LAYERS, D, QH * HD), D ** -0.5, 0.09375, ((0, 4), (2, 8))),
        "w_key": bell_draw(streams_of[4], (LAYERS, D, KVH * HD), D ** -0.5, 0.09375, ((0, 4), (2, 8))),
        "w_value": bell_draw(streams_of[5], (LAYERS, D, KVH * HD), D ** -0.5, 0.09375, ((0, 4), (2, 8))),
        "w_out": bell_draw(streams_of[6], (LAYERS, QH * HD, D), (QH * HD) ** -0.5, 0.125, ((0, 4), (1, 8))),
        "final_gain": jnp.clip(1.0 + 0.1 * jax.random.normal(streams_of[7], (D,), jnp.float32), 0.5, 1.5),
        "head_weight": draw_head_weight(jax.random.fold_in(streams_of[9], 71), part),
    }


EPSILON = 1e-05
ROPE_BASE = 500000.0

def normalize(states, gain_vec):
    values = states.astype(jnp.float32)
    return values * lax.rsqrt(lax.optimization_barrier(jnp.mean(values * values, axis=-1, keepdims=True)) + EPSILON) * gain_vec

def rotate(tensor, positions):
    half_dim = tensor.shape[-1] // 2
    index = jnp.arange(half_dim, dtype=jnp.float32)
    inverse = ROPE_BASE ** (-2.0 * index / tensor.shape[-1])
    angles = positions[:, None] * inverse[None, :]
    cosine = jnp.cos(angles)[:, None, :]
    sine = jnp.sin(angles)[:, None, :]
    first_half = tensor[..., :half_dim]
    second_half = tensor[..., half_dim:]
    return jnp.concatenate([first_half * cosine - second_half * sine, second_half * cosine + first_half * sine], axis=-1)

def project(normed, layer_query, layer_key, layer_value):
    n_rows = normed.shape[0]
    positions = jnp.arange(n_rows).astype(jnp.float32)
    query = jnp.dot(normed, layer_query, preferred_element_type=jnp.float32)
    query = rotate(query.reshape(n_rows, -1, HD), positions).reshape(n_rows, -1)
    keys = jnp.dot(normed, layer_key, preferred_element_type=jnp.float32)
    keys = rotate(keys.reshape(n_rows, -1, HD), positions).reshape(n_rows, -1)
    values = jnp.dot(normed, layer_value, preferred_element_type=jnp.float32)
    return jnp.concatenate([query, keys, values], axis=1)

def attend(projected, heads_q, heads_kv):
    n_rows = projected.shape[0]
    q_width = heads_q * HD
    k_width = heads_kv * HD
    query = projected[:, :q_width].reshape(n_rows, heads_kv, heads_q // heads_kv, HD).astype(jnp.float32)
    keys = projected[:, q_width:q_width + k_width].reshape(n_rows, heads_kv, HD).astype(jnp.float32)
    values = projected[:, q_width + k_width:].reshape(n_rows, heads_kv, HD).astype(jnp.float32)
    logits = jnp.einsum('skgd,tkd->kgst', query, keys) / math.sqrt(HD)
    causal = jnp.arange(n_rows)[:, None] >= jnp.arange(n_rows)[None, :]
    weights_attn = jax.nn.softmax(jnp.where(causal, logits, -1e+30), axis=-1).astype(jnp.bfloat16)
    context = jnp.einsum('kgst,tkd->skgd', weights_attn.astype(jnp.float32), values)
    return context.astype(jnp.bfloat16).reshape(n_rows, q_width)

def reference(embeds, labels, norm_gain, w_query, w_key, w_value, w_out, final_gain, head_weight):
    group_width = QH * HD // N_TENSOR
    states = [embeds[seq_index] for seq_index in range(MICRO)]
    for layer in range(LAYERS):
        out_grouped = w_out[layer].reshape(N_TENSOR, group_width, D).astype(jnp.float32)
        updated = []
        for state in states:
            normed = normalize(state, norm_gain[layer]).astype(jnp.bfloat16)
            projected = project(normed, w_query[layer], w_key[layer], w_value[layer]).astype(jnp.bfloat16)
            context = attend(projected, QH, KVH)
            grouped = context.reshape(SEQ, N_TENSOR, group_width).astype(jnp.float32)
            partial_sums = jnp.einsum('snc,ncd->nsd', grouped, out_grouped)
            rounded = lax.optimization_barrier(partial_sums.astype(jnp.bfloat16))
            block = lax.optimization_barrier(jnp.sum(rounded.astype(jnp.float32), axis=0))
            updated.append((state.astype(jnp.float32) + block).astype(jnp.bfloat16))
        states = updated
    hidden = normalize(jnp.stack(states), final_gain).astype(jnp.bfloat16)
    flat_rows = hidden.reshape(MICRO * SEQ, D)
    logits = jnp.dot(flat_rows, head_weight, preferred_element_type=jnp.float32)
    peak_row = lax.optimization_barrier(jnp.max(logits, axis=-1, keepdims=True))
    log_norm = peak_row[:, 0] + jnp.log(lax.optimization_barrier(jnp.sum(jnp.exp(logits - peak_row), axis=-1)))
    flat_labels = labels.reshape(-1).astype(jnp.int32)
    target = jnp.take_along_axis(logits, flat_labels[:, None], axis=1)[:, 0]
    token_loss = (log_norm - target).reshape(MICRO, SEQ)
    onehot = flat_labels[:, None] == jnp.arange(VOCAB, dtype=jnp.int32)[None, :]
    errors = (jnp.exp(logits - log_norm[:, None]) - onehot.astype(jnp.float32)).astype(jnp.bfloat16)
    errors = errors.reshape(MICRO, SEQ, VOCAB).astype(jnp.float32)
    hidden_f = hidden.astype(jnp.float32)
    gram_err = jnp.einsum('bsv,btv->bst', errors, errors)
    gram_hid = jnp.einsum('bsd,btd->bst', hidden_f, hidden_f)
    totals = lax.optimization_barrier(jnp.sum(gram_err * gram_hid, axis=(1, 2)))
    scores = jnp.sqrt(totals) / SEQ
    return (token_loss, scores)
```

```python
import math

import jax
import jax.numpy as jnp
from jax import lax
from jax.sharding import PartitionSpec as P

HD = 128
EPSILON = 1e-05
ROPE_BASE = 500000.0
CORES = 2


def sent_to_all(value, axis):
    size = lax.axis_size(axis)
    return lax.all_to_all(
        jnp.broadcast_to(value[None], (size, *value.shape)), axis, 0, 0, tiled=True
    )


def core_swap(value):
    size = lax.axis_size("tensor")
    return lax.ppermute(value, "tensor", [(t, t ^ 1) for t in range(size)])


def chip_shift(value, by):
    size = lax.axis_size("tensor")
    return lax.ppermute(value, "tensor", [(t, (t + CORES * by) % size) for t in range(size)])


def hop(value):
    size = lax.axis_size("pipe")
    return lax.ppermute(value, "pipe", [(i, i + 1) for i in range(size - 1)])


def normalize(states, gain_vec):
    values = states.astype(jnp.float32)
    return (
        values * lax.rsqrt(jnp.mean(values * values, axis=-1, keepdims=True) + EPSILON) * gain_vec
    )


def rotate(tensor, cosine, sine):
    half = tensor.shape[-1] // 2
    first, second = tensor[..., :half], tensor[..., half:]
    return jnp.concatenate(
        [first * cosine - second * sine, second * cosine + first * sine], axis=-1
    )


def attend(rows, weights, cosine, sine, causal):
    w_q, w_k, w_v = weights
    heads = w_q.shape[1] // HD
    query = jnp.dot(rows, w_q, preferred_element_type=jnp.float32)
    keys = jnp.dot(rows, w_k, preferred_element_type=jnp.float32)
    values = jnp.dot(rows, w_v, preferred_element_type=jnp.float32).astype(jnp.bfloat16)
    keys = rotate(keys, cosine, sine).astype(jnp.bfloat16)
    outs = []
    for h in range(heads):
        q = rotate(query[:, h * HD : (h + 1) * HD], cosine, sine).astype(jnp.bfloat16)
        logits = lax.dot_general(
            q, keys, (((1,), (1,)), ((), ())), preferred_element_type=jnp.float32
        ) / math.sqrt(HD)
        probs = jax.nn.softmax(jnp.where(causal, logits, -1e30), axis=-1).astype(jnp.bfloat16)
        outs.append(jnp.dot(probs, values, preferred_element_type=jnp.float32))
    return jnp.concatenate(outs, axis=1).astype(jnp.bfloat16)


def per_device(embeds, labels, norm_gain, w_query, w_key, w_value, w_out, final_gain, head_weight):
    pipe_count = lax.axis_size("pipe")
    tensor_count = lax.axis_size("tensor")
    chips = tensor_count // CORES
    section = lax.axis_index("pipe")
    rank = lax.axis_index("tensor")
    chip, core = rank // CORES, rank % CORES
    micro, own_rows, width = embeds.shape
    chains = micro // CORES
    seq_len = own_rows * tensor_count
    block = own_rows * CORES

    own_w = (w_query[0], w_key[0], w_value[0])
    own_out = w_out[0]

    by_core = embeds.reshape(chains, CORES, own_rows, width)
    mine = jnp.where(core == 0, by_core[:, 0], by_core[:, 1])
    theirs = jnp.where(core == 0, by_core[:, 1], by_core[:, 0])
    start = jnp.concatenate([mine, core_swap(theirs)], axis=1)
    other_w = tuple(core_swap(w) for w in own_w)
    other_out = core_swap(own_out)

    at = jnp.arange(seq_len, dtype=jnp.int32)
    from_chip = (chip - at // block + chips) % chips
    from_core = (core + (at % block) // own_rows) % CORES
    place = from_chip * block + from_core * own_rows + at % own_rows
    half = HD // 2
    inverse = ROPE_BASE ** (-2.0 * jnp.arange(half, dtype=jnp.float32) / HD)
    angles = place.astype(jnp.float32)[:, None] * inverse[None, :]
    cosine, sine = jnp.cos(angles), jnp.sin(angles)
    causal = place[:, None] >= place[None, :]

    def gathered(rows):
        return jnp.concatenate([rows] + [chip_shift(rows, k) for k in range(1, chips)], axis=0)

    hiddens = []
    for j in range(chains):
        state = start[j]
        for layer in range(pipe_count):
            with jax.named_scope(f"chain{j}_layer{layer}"):
                normed = normalize(state, norm_gain[0]).astype(jnp.bfloat16)
                rows = gathered(normed)
                part = jnp.dot(
                    attend(rows, own_w, cosine, sine, causal),
                    own_out,
                    preferred_element_type=jnp.float32,
                ) + jnp.dot(
                    attend(rows, other_w, cosine, sine, causal),
                    other_out,
                    preferred_element_type=jnp.float32,
                )
                part = part.reshape(chips, block, width)
                total = state.astype(jnp.float32) + part[0]
                sent = part.astype(jnp.bfloat16)
                for k in range(1, chips):
                    total = total + chip_shift(sent[k], -k).astype(jnp.float32)
                state = total.astype(jnp.bfloat16)
                if layer + 1 < pipe_count:
                    state = hop(state)
        with jax.named_scope(f"chain{j}_final"):
            hidden = normalize(state, final_gain).astype(jnp.bfloat16)
            spread = hidden
            for p in range(pipe_count - 1):
                got = lax.ppermute(hidden, "pipe", [(pipe_count - 1, p)])
                spread = jnp.where(section == p, got, spread)
            full = gathered(spread)
            hiddens.append(jnp.stack([full, core_swap(full)]))

    with jax.named_scope("head"):
        hidden = jnp.stack(hiddens)
        logits = jnp.stack(
            [
                jnp.dot(
                    h.reshape(CORES * seq_len, width),
                    head_weight,
                    preferred_element_type=jnp.float32,
                ).reshape(CORES, seq_len, -1)
                for h in hiddens
            ]
        )
        vocab_dev = head_weight.shape[1]
        slot = section * tensor_count + rank
        swap_rows = lambda v: jnp.flip(
            v.reshape(*v.shape[:-1], chips, CORES, own_rows), axis=-2
        ).reshape(v.shape)

        def to_mine(v):
            v = v.reshape(chains, CORES, chips, CORES, own_rows)
            v = jnp.where(core == 0, v, v[:, ::-1])
            turned = [v[:, :, [(c - k) % chips for k in range(chips)]] for c in range(chips)]
            v = sum(jnp.where(chip == c, turned[c], 0) for c in range(chips))
            flip = v[:, :, :, ::-1]
            first = jnp.where(core == 0, v[:, :1], flip[:, :1])
            second = jnp.where(core == 0, flip[:, 1:], v[:, 1:])
            return jnp.concatenate([first, second], axis=1).reshape(chains, CORES, seq_len)

        def to_all(v):
            lead = v.shape[:-3]
            v = v.reshape(*lead, chains, CORES, chips, CORES, own_rows)
            flip = v[..., ::-1, :]
            first = jnp.where(core == 0, v[..., :1, :, :, :], flip[..., :1, :, :, :])
            second = jnp.where(core == 0, flip[..., 1:, :, :, :], v[..., 1:, :, :, :])
            v = jnp.concatenate([first, second], axis=-4)
            turned = [v[..., [(c - k) % chips for k in range(chips)], :, :] for c in range(chips)]
            v = sum(jnp.where(chip == c, turned[c], 0) for c in range(chips))
            v = jnp.where(core == 0, v, jnp.flip(v, axis=-4))
            return v.reshape(*lead, micro, seq_len)

        local_ids = to_mine(labels) - slot * vocab_dev
        onehot = local_ids[..., None] == jnp.arange(vocab_dev, dtype=jnp.int32)
        target_local = jnp.sum(jnp.where(onehot, logits, 0.0), axis=-1)
        peak_local = jnp.max(logits, axis=-1)
        relative = jnp.sum(jnp.exp(logits - peak_local[..., None]), axis=-1)
        stats = to_all(jnp.stack([peak_local, relative, target_local]))
        stats = sent_to_all(stats.reshape(3, micro * seq_len), ("pipe", "tensor"))
        peak = jnp.max(stats[:, 0], axis=0)
        exp_total = jnp.sum(stats[:, 1] * jnp.exp(stats[:, 0] - peak), axis=0)
        target = jnp.sum(stats[:, 2], axis=0)
        log_norm = (peak + jnp.log(exp_total)).reshape(micro, seq_len)
        losses = log_norm - target.reshape(micro, seq_len)
        errors = (
            jnp.exp(logits - to_mine(log_norm)[..., None]) - onehot.astype(jnp.float32)
        ).astype(jnp.bfloat16)
        gram_err = jnp.einsum("bcsv,bctv->bcst", errors, errors, preferred_element_type=jnp.float32)
        gram_hid = jnp.einsum("bcsd,bctd->bcst", hidden, hidden, preferred_element_type=jnp.float32)
        parts = jnp.sum(gram_err * gram_hid, axis=(2, 3))
        parts = jnp.where(core == 0, parts, parts[:, ::-1]).reshape(micro)
        totals = sent_to_all(parts[None], ("pipe", "tensor")).sum(axis=(0, 1))
        scores = jnp.sqrt(totals) / seq_len
        loss_width = seq_len // (pipe_count * tensor_count)
        token_loss = lax.dynamic_slice_in_dim(losses, slot * loss_width, loss_width, 1)
    return (token_loss, scores)


def solution(mesh):
    in_specs = (
        P("dp", "tensor", None),
        P("dp", None),
        P("pipe", None),
        P("pipe", None, "tensor"),
        P("pipe", None, "tensor"),
        P("pipe", None, "tensor"),
        P("pipe", "tensor", None),
        P(),
        P(None, ("pipe", "tensor")),
    )
    out_specs = (P("dp", ("pipe", "tensor")), P("dp"))
    return jax.shard_map(
        per_device, mesh=mesh, in_specs=in_specs, out_specs=out_specs, check_vma=False
    )
```

```python
import functools
import math

import jax
import jax.numpy as jnp
from jax import lax
from jax.experimental import pallas as pl
from jax.experimental.pallas import tpu as pltpu
from jax.sharding import PartitionSpec as P

HD = 128
EPSILON = 1e-05
ROPE_BASE = 500000.0
CORES = 2
MIB = 1024 * 1024
F32, BF16 = jnp.float32, jnp.bfloat16
IN_VMEM = pl.BlockSpec(memory_space=pltpu.VMEM)
IN_SMEM = pl.BlockSpec(memory_space=pltpu.SMEM)
IN_HBM = pl.BlockSpec(memory_space=pltpu.HBM)


def sent_to_all(value, axis):
    size = lax.axis_size(axis)
    return lax.all_to_all(
        jnp.broadcast_to(value[None], (size, *value.shape)), axis, 0, 0, tiled=True
    )


def core_swap(value):
    size = lax.axis_size("tensor")
    return lax.ppermute(value, "tensor", [(t, t ^ 1) for t in range(size)])


def chip_shift(value, by):
    size = lax.axis_size("tensor")
    return lax.ppermute(value, "tensor", [(t, (t + CORES * by) % size) for t in range(size)])


def hop(value):
    size = lax.axis_size("pipe")
    return lax.ppermute(value, "pipe", [(i, i + 1) for i in range(size - 1)])


def normalize(states, gain_vec):
    values = states.astype(F32)
    return (
        values * lax.rsqrt(jnp.mean(values * values, axis=-1, keepdims=True) + EPSILON) * gain_vec
    )


def loader_kernel(*refs, plan):
    n_in = len(plan)
    ins, outs, sems = refs[:n_in], refs[n_in:-1], refs[-1]
    copies = []
    for i, (out, at) in enumerate(plan):
        target = outs[out].at[:, at : at + ins[i].shape[1]]
        copies.append(pltpu.make_async_copy(ins[i], target, sems.at[i]))
    for c in copies:
        c.start()
    for c in copies:
        c.wait()


def resident(groups, room):
    flat = [w for group in groups for w in group]
    plan, shapes = [], []
    for out, group in enumerate(groups):
        at = 0
        for w in group:
            plan.append((out, at))
            at += w.shape[1]
        shapes.append(pltpu.VMEM((group[0].shape[0], at), BF16))
    return pl.pallas_call(
        functools.partial(loader_kernel, plan=plan),
        out_shape=shapes,
        in_specs=[IN_HBM] * len(flat),
        out_specs=[IN_VMEM] * len(groups),
        scratch_shapes=[pltpu.SemaphoreType.DMA((len(flat),))],
        cost_estimate=pl.CostEstimate(
            flops=10**9, bytes_accessed=4 * sum(w.size for w in flat), transcendentals=0
        ),
        compiler_params=pltpu.CompilerParams(vmem_limit_bytes=room * MIB),
        name="resident",
    )(*flat)


def section_kernel(
    r0, r1, r2, r3, state, wa, oa, wb, ob, cos_ref, sin_ref, bias_ref, p0, p1, p2, p3
):
    rows = jnp.concatenate([r0[...], r1[...], r2[...], r3[...]], axis=0)
    cosine, sine, bias = cos_ref[...], sin_ref[...], bias_ref[...]
    n_rows = rows.shape[0]

    def rotated(t):
        return (t * cosine + pltpu.roll(t, HD // 2, 1) * sine).astype(BF16)

    contexts = []
    for w in (wa, wb):
        both = jnp.dot(rows, w[...], preferred_element_type=F32)
        heads = both.shape[1] // HD - 2
        keys = rotated(both[:, heads * HD : (heads + 1) * HD])
        values = both[:, (heads + 1) * HD :].astype(BF16)
        stacked = jnp.concatenate(
            [rotated(both[:, h * HD : (h + 1) * HD]) for h in range(heads)], axis=0
        )
        logits = lax.dot_general(
            stacked, keys, (((1,), (1,)), ((), ())), preferred_element_type=F32
        ) / math.sqrt(HD)
        logits = logits + bias
        weights = jnp.exp(logits - jnp.max(logits, axis=-1, keepdims=True))
        probs = (weights / jnp.sum(weights, axis=-1, keepdims=True)).astype(BF16)
        out = jnp.dot(probs, values, preferred_element_type=F32).astype(BF16)
        contexts.append(
            jnp.concatenate([out[h * n_rows : (h + 1) * n_rows] for h in range(heads)], axis=1)
        )
    block = r0.shape[0]
    width = oa.shape[1]
    step = 512
    for n in range(0, width, step):
        cols = slice(n, n + step)
        part = jnp.dot(contexts[0], oa[:, cols], preferred_element_type=F32) + jnp.dot(
            contexts[1], ob[:, cols], preferred_element_type=F32
        )
        p0[:, cols] = part[:block] + state[:, cols].astype(F32)
        for i, p in ((1, p1), (2, p2), (3, p3)):
            p[:, cols] = part[i * block : (i + 1) * block].astype(BF16)


def section_block(blocks, state, own, other, cosine, sine, bias):
    block, width = state.shape
    shapes = [jax.ShapeDtypeStruct((block, width), F32)] + [
        jax.ShapeDtypeStruct((block, width), BF16)
    ] * 3
    return pl.pallas_call(
        section_kernel,
        out_shape=shapes,
        in_specs=[IN_VMEM] * 12,
        out_specs=[IN_VMEM] * 4,
        cost_estimate=pl.CostEstimate(
            flops=8 * 10**9, bytes_accessed=2 * width * 1536, transcendentals=0
        ),
        compiler_params=pltpu.CompilerParams(vmem_limit_bytes=16 * MIB),
        name="section_block",
    )(*blocks, state, *own, *other, cosine, sine, bias)


def as_column(row):
    n = row.shape[1]
    return jnp.transpose(jnp.broadcast_to(row, (n, n)))[:, :1]


def head_kernel(
    at_ref, b0, b1, b2, b3, s0, s1, s2, s3, w_ref, ids_ref, logits_ref, stats_ref, gram_ref, hidden
):
    chip, core = at_ref[0], at_ref[1]
    block = b0.shape[0]
    chips = 4
    for side, group in ((core, (b0, b1, b2, b3)), (1 - core, (s0, s1, s2, s3))):
        for k, b in enumerate(group):
            row = (side * chips + lax.rem(chip - k + chips, chips)) * block
            hidden[pl.ds(pl.multiple_of(row, block), block), :] = b[...]
    logits = jnp.dot(hidden[...], w_ref[...], preferred_element_type=F32)
    logits_ref[...] = logits
    n_rows, vocab = logits.shape
    hit = as_column(ids_ref[...]) == lax.broadcasted_iota(jnp.int32, (n_rows, vocab), 1).astype(F32)
    target = jnp.sum(jnp.where(hit, logits, 0.0), axis=1, keepdims=True)
    peak = jnp.max(logits, axis=1, keepdims=True)
    total = jnp.sum(jnp.exp(logits - peak), axis=1, keepdims=True)
    lane = lax.broadcasted_iota(jnp.int32, (n_rows, n_rows), 1)
    table = jnp.where(lane == 0, peak, jnp.where(lane == 1, total, target))
    stats_ref[...] = jnp.transpose(table)[:8]
    seq = n_rows // CORES
    for i in range(CORES):
        h = hidden[i * seq : (i + 1) * seq, :]
        gram_ref[i] = lax.dot_general(h, h, (((1,), (1,)), ((), ())), preferred_element_type=F32)


def head_block(where, mine, theirs, head_weight, ids):
    block, width = mine[0].shape
    n_rows, vocab = 2 * len(mine) * block, head_weight.shape[1]
    seq = n_rows // CORES
    return pl.pallas_call(
        head_kernel,
        out_shape=[
            jax.ShapeDtypeStruct((n_rows, vocab), F32),
            jax.ShapeDtypeStruct((8, n_rows), F32),
            jax.ShapeDtypeStruct((CORES, seq, seq), F32),
        ],
        in_specs=[IN_SMEM] + [IN_VMEM] * 10,
        out_specs=[IN_VMEM] * 3,
        scratch_shapes=[pltpu.VMEM((n_rows, width), BF16)],
        cost_estimate=pl.CostEstimate(
            flops=4 * 10**9, bytes_accessed=2 * width * vocab, transcendentals=0
        ),
        compiler_params=pltpu.CompilerParams(vmem_limit_bytes=16 * MIB),
        name="head_block",
    )(where, *mine, *theirs, head_weight, ids)


def score_kernel(l0, l1, norm_ref, i0, i1, g0, g1, out_ref):
    chain_rows, vocab = l0.shape
    seq = chain_rows // CORES
    lane = lax.broadcasted_iota(jnp.int32, (8, 128), 1)
    result = jnp.zeros((8, 128), F32)
    for j, (logits, ids, gram) in enumerate(((l0, i0, g0), (l1, i1, g1))):
        norm = as_column(norm_ref[:, j * chain_rows : (j + 1) * chain_rows])
        entry = lax.broadcasted_iota(jnp.int32, (chain_rows, vocab), 1).astype(F32)
        hit = as_column(ids[...]) == entry
        errors = jnp.exp(logits[...] - norm) - hit.astype(F32)
        errors = errors.astype(BF16)
        for i in range(CORES):
            e = errors[i * seq : (i + 1) * seq]
            pair = lax.dot_general(e, e, (((1,), (1,)), ((), ())), preferred_element_type=F32)
            result = jnp.where(lane == j * CORES + i, jnp.sum(pair * gram[i]), result)
    out_ref[...] = result


def score_block(logits, log_norm, ids, grams):
    return pl.pallas_call(
        score_kernel,
        out_shape=jax.ShapeDtypeStruct((8, 128), F32),
        in_specs=[IN_VMEM] * 7,
        out_specs=IN_VMEM,
        cost_estimate=pl.CostEstimate(flops=10**9, bytes_accessed=10**6, transcendentals=0),
        compiler_params=pltpu.CompilerParams(vmem_limit_bytes=12 * MIB),
        name="score_block",
    )(*logits, log_norm, *ids, *grams)


def per_device(embeds, labels, norm_gain, w_query, w_key, w_value, w_out, final_gain, head_weight):
    pipe_count = lax.axis_size("pipe")
    tensor_count = lax.axis_size("tensor")
    chips = tensor_count // CORES
    section = lax.axis_index("pipe")
    rank = lax.axis_index("tensor")
    chip, core = rank // CORES, rank % CORES
    micro, own_rows, width = embeds.shape
    chains = micro // CORES
    seq_len = own_rows * tensor_count
    block = own_rows * CORES

    own_w = (w_query[0], w_key[0], w_value[0], w_out[0])
    vocab_dev = head_weight.shape[1]
    slot = section * tensor_count + rank
    loss_width = seq_len // (pipe_count * tensor_count)
    at_section = [section == p for p in range(pipe_count - 1)]
    scalars = (core == 0, at_section, slot * vocab_dev, slot * loss_width, chip, core)
    embeds, scalars = lax.optimization_barrier((embeds, scalars))
    on_first, at_section, first_id, loss_at, chip, core = scalars
    ids = (labels - first_id).astype(F32).reshape(chains, 1, CORES * seq_len)
    where = jnp.stack([chip, core]).astype(jnp.int32)

    by_core = embeds.reshape(chains, CORES, own_rows, width)
    mine = jnp.where(on_first, by_core[:, 0], by_core[:, 1])
    got = core_swap(jnp.where(on_first, by_core[:, 1], by_core[:, 0]))
    start = jnp.where(
        on_first, jnp.concatenate([mine, got], axis=1), jnp.concatenate([got, mine], axis=1)
    )
    other_w = tuple(core_swap(w) for w in own_w)
    at = jnp.arange(seq_len, dtype=jnp.int32)
    place = (chip - at // block + chips) % chips * block + at % block
    half = HD // 2
    inverse = ROPE_BASE ** (-2.0 * jnp.arange(half, dtype=F32) / HD)
    angles = place.astype(F32)[:, None] * inverse[None, :]
    cosine, sine = jnp.cos(angles), jnp.sin(angles)
    cosine = jnp.concatenate([cosine, cosine], axis=1)
    sine = jnp.concatenate([-sine, sine], axis=1)
    bias = jnp.where(place[:, None] >= place[None, :], 0.0, -1e30)
    bias = jnp.concatenate([bias] * (own_w[0].shape[1] // HD), axis=0)

    def gathered(rows):
        return [rows] + [chip_shift(rows, k) for k in range(1, chips)]

    normed = normalize(start[0], norm_gain[0]).astype(BF16)
    held = lax.optimization_barrier((own_w, head_weight, [*ids], where, normed))
    loaded_w, loaded_head, ids, where, normed = held
    *own, head_w = resident([loaded_w[:3], loaded_w[3:], [loaded_head]], 50)
    other = resident([other_w[:3], other_w[3:]], 16)

    def section_tick(state, normed, tick, beside=(), after=()):
        with jax.named_scope(f"tick{tick}"):
            blocks = gathered(normed)
            blocks, beside = lax.optimization_barrier((blocks, beside))
            after = after(beside) if after else ()
            parts = section_block(blocks, state, own, other, cosine, sine, bias)
            got = [chip_shift(parts[k], -k) for k in range(1, chips)]
            got, after = lax.optimization_barrier((got, after))
            total = parts[0]
            for g in got:
                total = total + g.astype(F32)
            return total.astype(BF16), after

    def next_state(result, tick):
        with jax.named_scope(f"hop{tick}"):
            state = hop(result)
            if tick < chains:
                state = jnp.where(at_section[0], start[tick], state)
            return state, normalize(state, norm_gain[0]).astype(BF16)

    def spread_of(result, j):
        with jax.named_scope(f"spread{j}"):
            hidden = normalize(result, final_gain).astype(BF16)
            here = [
                lax.ppermute(hidden, "pipe", [(pipe_count - 1, p)]) for p in range(pipe_count - 1)
            ]
            spread = hidden
            for p in range(pipe_count - 1):
                spread = jnp.where(at_section[p], here[p], spread)
            return spread

    state = start[0]
    result, _ = section_tick(state, normed, 0)
    ticks = chains + pipe_count - 1
    heads = []
    for tick in range(1, ticks):
        state, normed = next_state(result, tick)
        if tick < ticks - 1:
            result, _ = section_tick(state, normed, tick)
            continue
        done, normed = lax.optimization_barrier((result, normed))
        spread = spread_of(done, 0)
        result, blocks = section_tick(
            state, normed, tick, beside=spread, after=lambda s: gathered(s)
        )
        with jax.named_scope("head0"):
            theirs = [core_swap(b) for b in blocks]
            first = (blocks, theirs)
    spread = spread_of(result, 1)
    spread, first = lax.optimization_barrier((spread, first))
    heads.append(head_block(where, *first, head_w, ids[0]))
    with jax.named_scope("head1"):
        blocks = gathered(spread)
        blocks, heads = lax.optimization_barrier((blocks, heads))
        theirs = [core_swap(b) for b in blocks]
        heads.append(head_block(where, blocks, theirs, head_w, ids[1]))

    with jax.named_scope("scores"):
        stats = jnp.concatenate([h[1] for h in heads], axis=1)[:3]
        stats = sent_to_all(stats, ("pipe", "tensor"))
        peak = jnp.max(stats[:, 0], axis=0)
        exp_total = jnp.sum(stats[:, 1] * jnp.exp(stats[:, 0] - peak), axis=0)
        target = jnp.sum(stats[:, 2], axis=0)
        log_norm = peak + jnp.log(exp_total)
        parts = score_block(
            [h[0] for h in heads], log_norm[None], ids, [h[2] for h in heads]
        )
        totals = sent_to_all(parts[:1, :micro], ("pipe", "tensor")).sum(axis=(0, 1))
        scores = jnp.sqrt(totals) / seq_len
        losses = (log_norm - target).reshape(micro, seq_len)
        token_loss = lax.dynamic_slice(
            losses, (0, loss_at), (micro, loss_width), allow_negative_indices=False
        )
    return (token_loss, scores)


def solution(mesh):
    in_specs = (
        P("dp", "tensor", None),
        P("dp", None),
        P("pipe", None),
        P("pipe", None, "tensor"),
        P("pipe", None, "tensor"),
        P("pipe", None, "tensor"),
        P("pipe", "tensor", None),
        P(),
        P(None, ("pipe", "tensor")),
    )
    out_specs = (P("dp", ("pipe", "tensor")), P("dp"))
    return jax.shard_map(
        per_device, mesh=mesh, in_specs=in_specs, out_specs=out_specs, check_vma=False
    )
```

```python
import functools
import math

import jax
import jax.numpy as jnp
from jax import lax
from jax.experimental import pallas as pl
from jax.experimental.pallas import tpu as pltpu
from jax.sharding import PartitionSpec as P

HD = 128
EPSILON = 1e-05
ROPE_BASE = 500000.0
CORES = 2
MIB = 1024 * 1024
F32, BF16 = jnp.float32, jnp.bfloat16
IN_VMEM = pl.BlockSpec(memory_space=pltpu.VMEM)
IN_SMEM = pl.BlockSpec(memory_space=pltpu.SMEM)
IN_HBM = pl.BlockSpec(memory_space=pltpu.HBM)


def sent_to_all(value, axis):
    size = lax.axis_size(axis)
    return lax.all_to_all(
        jnp.broadcast_to(value[None], (size, *value.shape)), axis, 0, 0, tiled=True
    )


def core_swap(value):
    size = lax.axis_size("tensor")
    return lax.ppermute(value, "tensor", [(t, t ^ 1) for t in range(size)])


def chip_swap(value, k):
    size = lax.axis_size("tensor")
    return lax.ppermute(value, "tensor", [(t, t ^ (CORES * k)) for t in range(size)])


def hop(value):
    size = lax.axis_size("pipe")
    return lax.ppermute(value, "pipe", [(i, i + 1) for i in range(size - 1)])


def normalize(states, gain_vec):
    values = states.astype(F32)
    return (
        values * lax.rsqrt(jnp.mean(values * values, axis=-1, keepdims=True) + EPSILON) * gain_vec
    )


def loader_kernel(*refs, plan):
    n_in = len(plan)
    ins, outs, sems = refs[:n_in], refs[n_in:-1], refs[-1]
    copies = []
    for i, (out, side, at) in enumerate(plan):
        target = outs[out].at[side, :, at : at + ins[i].shape[1]]
        copies.append(pltpu.make_async_copy(ins[i], target, sems.at[i]))
    for c in copies:
        c.start()
    for c in copies:
        c.wait()


def resident(arrays, room):
    flat = [w for sides in arrays for parts in sides for w in parts]
    plan, shapes = [], []
    for out, sides in enumerate(arrays):
        for side, parts in enumerate(sides):
            at = 0
            for w in parts:
                plan.append((out, side, at))
                at += w.shape[1]
        shapes.append(pltpu.VMEM((len(sides), sides[0][0].shape[0], at), BF16))
    return pl.pallas_call(
        functools.partial(loader_kernel, plan=plan),
        out_shape=shapes,
        in_specs=[IN_HBM] * len(flat),
        out_specs=[IN_VMEM] * len(shapes),
        scratch_shapes=[pltpu.SemaphoreType.DMA((len(flat),))],
        cost_estimate=pl.CostEstimate(
            flops=10**9, bytes_accessed=4 * sum(w.size for w in flat), transcendentals=0
        ),
        compiler_params=pltpu.CompilerParams(vmem_limit_bytes=room * MIB),
        name="resident",
    )(*flat)


def section_body(rows, context, state, w_in, w_out, cos_ref, sin_ref, bias_ref, outs):
    cosine, sine, bias = cos_ref[...], sin_ref[...], bias_ref[...]
    n_rows = rows.shape[0]
    sides, depth, _ = w_out.shape

    def rotated(t):
        return (t * cosine + pltpu.roll(t, HD // 2, 1) * sine).astype(BF16)

    def attend(side, carry):
        both = jnp.dot(rows[...], w_in[side], preferred_element_type=F32)
        heads = both.shape[1] // HD - 2
        keys = rotated(both[:, heads * HD : (heads + 1) * HD])
        values = both[:, (heads + 1) * HD :].astype(BF16)
        stacked = jnp.concatenate(
            [rotated(both[:, h * HD : (h + 1) * HD]) for h in range(heads)], axis=0
        )
        logits = lax.dot_general(
            stacked, keys, (((1,), (1,)), ((), ())), preferred_element_type=F32
        ) / math.sqrt(HD)
        logits = logits + bias
        weights = jnp.exp(logits - jnp.max(logits, axis=-1, keepdims=True))
        probs = (weights / jnp.sum(weights, axis=-1, keepdims=True)).astype(BF16)
        out = jnp.dot(probs, values, preferred_element_type=F32).astype(BF16)
        context[side] = jnp.concatenate(
            [out[h * n_rows : (h + 1) * n_rows] for h in range(heads)], axis=1
        )
        return carry

    lax.fori_loop(0, sides, attend, 0)
    block, width = outs[0].shape
    step = width // 2

    def columns(c, carry):
        cols = pl.ds(pl.multiple_of(c * step, step), step)
        part = sum(
            jnp.dot(context[i], w_out[i, :, cols], preferred_element_type=F32)
            for i in range(sides)
        )
        outs[0][:, cols] = part[:block] + state[:, cols].astype(F32)
        for i in range(1, len(outs)):
            outs[i][:, cols] = part[i * block : (i + 1) * block].astype(BF16)
        return carry

    lax.fori_loop(0, width // step, columns, 0)


def section_kernel(r0, r1, r2, r3, state, *rest):
    *rest, rows, context = rest
    block = r0.shape[0]
    for i, r in enumerate((r0, r1, r2, r3)):
        rows[i * block : (i + 1) * block, :] = r[...]
    section_body(rows, context, state, *rest[:5], rest[5:])


def first_kernel(at_ref, whole, gain_ref, *rest):
    *rest, rows, context, state = rest
    chips = 4
    block = whole.shape[0] // chips
    for k in range(chips):
        row = jnp.bitwise_xor(at_ref[0], k) * block
        values = whole[pl.ds(pl.multiple_of(row, block), block), :]
        if k == 0:
            state[...] = values
        values = values.astype(F32)
        mean = jnp.mean(values * values, axis=-1, keepdims=True)
        normed = values * lax.rsqrt(mean + EPSILON) * gain_ref[...]
        rows[k * block : (k + 1) * block, :] = normed.astype(BF16)
    section_body(rows, context, state, *rest[:5], rest[5:])


def section_block(kernel, specs, entering, block, width, held, tables, scratch=()):
    shapes = [jax.ShapeDtypeStruct((block, width), F32)] + [
        jax.ShapeDtypeStruct((block, width), BF16)
    ] * 3
    n_rows = tables[0].shape[0]
    sides, depth, _ = held[1].shape
    return pl.pallas_call(
        kernel,
        out_shape=shapes,
        in_specs=specs + [IN_VMEM] * 5,
        out_specs=[IN_VMEM] * 4,
        scratch_shapes=[
            pltpu.VMEM((n_rows, width), BF16),
            pltpu.VMEM((sides, n_rows, depth), BF16),
            *scratch,
        ],
        cost_estimate=pl.CostEstimate(
            flops=8 * 10**9, bytes_accessed=2 * width * 1536, transcendentals=0
        ),
        compiler_params=pltpu.CompilerParams(vmem_limit_bytes=16 * MIB),
        name="section_block",
    )(*entering, *held, *tables)


def as_column(row):
    n = row.shape[1]
    return jnp.transpose(jnp.broadcast_to(row, (n, n)))[:, :1]


def head_kernel(
    at_ref, mine, theirs, w_ref, ids_ref, logits_ref, stats_ref, gram_ref, hidden
):
    chip, core = at_ref[0], at_ref[1]
    chips = 4
    block = mine.shape[0] // chips
    for side, rows in ((core, mine), (1 - core, theirs)):
        for k in range(chips):
            row = (side * chips + jnp.bitwise_xor(chip, k)) * block
            target = pl.ds(pl.multiple_of(row, block), block)
            hidden[target, :] = rows[k * block : (k + 1) * block, :]
    step = 256

    def columns(c, carry):
        cols = pl.ds(pl.multiple_of(c * step, step), step)
        logits_ref[:, cols] = jnp.dot(hidden[...], w_ref[0, :, cols], preferred_element_type=F32)
        return carry

    lax.fori_loop(0, w_ref.shape[2] // step, columns, 0)
    logits = logits_ref[...]
    n_rows, vocab = logits.shape
    hit = as_column(ids_ref[...]) == lax.broadcasted_iota(jnp.int32, (n_rows, vocab), 1).astype(F32)
    target = jnp.sum(jnp.where(hit, logits, 0.0), axis=1, keepdims=True)
    peak = jnp.max(logits, axis=1, keepdims=True)
    total = jnp.sum(jnp.exp(logits - peak), axis=1, keepdims=True)
    lane = lax.broadcasted_iota(jnp.int32, (n_rows, n_rows), 1)
    table = jnp.where(lane == 0, peak, jnp.where(lane == 1, total, target))
    stats_ref[...] = jnp.transpose(table)[:8]
    seq = n_rows // CORES
    for i in range(CORES):
        h = hidden[i * seq : (i + 1) * seq, :]
        gram_ref[i] = lax.dot_general(h, h, (((1,), (1,)), ((), ())), preferred_element_type=F32)


def head_block(where, mine, theirs, head_weight, ids):
    seq, width = mine.shape
    n_rows, vocab = CORES * seq, head_weight.shape[2]
    return pl.pallas_call(
        head_kernel,
        out_shape=[
            jax.ShapeDtypeStruct((n_rows, vocab), F32),
            jax.ShapeDtypeStruct((8, n_rows), F32),
            jax.ShapeDtypeStruct((CORES, seq, seq), F32),
        ],
        in_specs=[IN_SMEM] + [IN_VMEM] * 4,
        out_specs=[IN_VMEM] * 3,
        scratch_shapes=[pltpu.VMEM((n_rows, width), BF16)],
        cost_estimate=pl.CostEstimate(
            flops=4 * 10**9, bytes_accessed=2 * width * vocab, transcendentals=0
        ),
        compiler_params=pltpu.CompilerParams(vmem_limit_bytes=16 * MIB),
        name="head_block",
    )(where, mine, theirs, head_weight, ids)


def score_kernel(l0, l1, norm_ref, i0, i1, g0, g1, out_ref):
    chain_rows, vocab = l0.shape
    seq = chain_rows // CORES
    lane = lax.broadcasted_iota(jnp.int32, (8, 128), 1)
    result = jnp.zeros((8, 128), F32)
    for j, (logits, ids, gram) in enumerate(((l0, i0, g0), (l1, i1, g1))):
        norm = as_column(norm_ref[:, j * chain_rows : (j + 1) * chain_rows])
        entry = lax.broadcasted_iota(jnp.int32, (chain_rows, vocab), 1).astype(F32)
        hit = as_column(ids[...]) == entry
        errors = jnp.exp(logits[...] - norm) - hit.astype(F32)
        errors = errors.astype(BF16)
        for i in range(CORES):
            e = errors[i * seq : (i + 1) * seq]
            pair = lax.dot_general(e, e, (((1,), (1,)), ((), ())), preferred_element_type=F32)
            result = jnp.where(lane == j * CORES + i, jnp.sum(pair * gram[i]), result)
    out_ref[...] = result


def score_block(logits, log_norm, ids, grams):
    return pl.pallas_call(
        score_kernel,
        out_shape=jax.ShapeDtypeStruct((8, 128), F32),
        in_specs=[IN_VMEM] * 7,
        out_specs=IN_VMEM,
        cost_estimate=pl.CostEstimate(flops=10**9, bytes_accessed=10**6, transcendentals=0),
        compiler_params=pltpu.CompilerParams(vmem_limit_bytes=12 * MIB),
        name="score_block",
    )(*logits, log_norm, *ids, *grams)


def per_device(embeds, labels, norm_gain, w_query, w_key, w_value, w_out, final_gain, head_weight):
    pipe_count = lax.axis_size("pipe")
    tensor_count = lax.axis_size("tensor")
    chips = tensor_count // CORES
    section = lax.axis_index("pipe")
    rank = lax.axis_index("tensor")
    chip, core = rank // CORES, rank % CORES
    micro, own_rows, width = embeds.shape
    chains = micro // CORES
    seq_len = own_rows * tensor_count
    block = own_rows * CORES

    own_w = (w_query[0], w_key[0], w_value[0], w_out[0])
    vocab_dev = head_weight.shape[1]
    slot = section * tensor_count + rank
    loss_width = seq_len // (pipe_count * tensor_count)
    at_section = [section == p for p in range(pipe_count - 1)]
    scalars = (core == 0, at_section, slot * vocab_dev, slot * loss_width, chip, core)
    embeds, scalars = lax.optimization_barrier((embeds, scalars))
    on_first, at_section, first_id, loss_at, chip, core = scalars
    ids = (labels - first_id).astype(F32).reshape(chains, 1, CORES * seq_len)
    where = jnp.stack([chip, core]).astype(jnp.int32)

    first_rows = jnp.broadcast_to(embeds[:CORES][None], (chips, CORES, own_rows, width))
    first_rows = first_rows.reshape(tensor_count, own_rows, width)
    whole = lax.all_to_all(first_rows, "tensor", 0, 0, tiled=True).reshape(seq_len, width)
    other_w = [core_swap(w) for w in own_w]

    later = embeds[CORES:].reshape(chains - 1, CORES, own_rows, width)
    mine = jnp.where(on_first, later[:, 0], later[:, 1])
    got = core_swap(jnp.where(on_first, later[:, 1], later[:, 0]))
    start = jnp.where(
        on_first, jnp.concatenate([mine, got], axis=1), jnp.concatenate([got, mine], axis=1)
    )

    at = jnp.arange(seq_len, dtype=jnp.int32)
    place = jnp.bitwise_xor(chip, at // block) * block + at % block
    half = HD // 2
    inverse = ROPE_BASE ** (-2.0 * jnp.arange(half, dtype=F32) / HD)
    angles = place.astype(F32)[:, None] * inverse[None, :]
    cosine, sine = jnp.cos(angles), jnp.sin(angles)
    cosine = jnp.concatenate([cosine, cosine], axis=1)
    sine = jnp.concatenate([-sine, sine], axis=1)
    bias = jnp.where(place[:, None] >= place[None, :], 0.0, -1e30)
    bias = jnp.concatenate([bias] * (own_w[0].shape[1] // HD), axis=0)

    def gathered(rows):
        return [rows] + [chip_swap(rows, k) for k in range(1, chips)]

    tables = (cosine, sine, bias)
    ready = lax.optimization_barrier((whole, [*ids], where, tables, own_w))
    whole, ids, where, tables, own_w = ready
    held = resident(
        [[own_w[:3], other_w[:3]], [own_w[3:], other_w[3:]]],
        48,
    )

    def summed(parts, after=()):
        got = [chip_swap(parts[k], k) for k in range(1, chips)]
        got, after = lax.optimization_barrier((got, after))
        total = parts[0]
        for g in got:
            total = total + g.astype(F32)
        return total.astype(BF16), after

    def section_tick(state, normed, tick, beside=(), after=()):
        with jax.named_scope(f"tick{tick}"):
            blocks = gathered(normed)
            blocks, beside = lax.optimization_barrier((blocks, beside))
            after = after(beside) if after else ()
            parts = section_block(
                section_kernel,
                [IN_VMEM] * 5,
                (*blocks, state),
                block,
                width,
                held,
                tables,
            )
            return (*summed(parts, after), beside)

    def next_state(result, tick):
        with jax.named_scope(f"hop{tick}"):
            state = hop(result)
            if tick < chains:
                state = jnp.where(at_section[0], start[tick - 1], state)
            return state, normalize(state, norm_gain[0]).astype(BF16)

    def spread_of(result, j):
        with jax.named_scope(f"spread{j}"):
            hidden = normalize(result, final_gain).astype(BF16)
            here = [
                lax.ppermute(hidden, "pipe", [(pipe_count - 1, p)]) for p in range(pipe_count - 1)
            ]
            spread = hidden
            for p in range(pipe_count - 1):
                spread = jnp.where(at_section[p], here[p], spread)
            return spread

    with jax.named_scope("tick0"):
        parts = section_block(
            first_kernel,
            [IN_SMEM, IN_VMEM, IN_VMEM],
            (where, whole, norm_gain),
            block,
            width,
            held,
            tables,
            scratch=[pltpu.VMEM((block, width), BF16)],
        )
        result, _ = summed(parts)
    ticks = chains + pipe_count - 1
    heads = []
    for tick in range(1, ticks):
        state, normed = next_state(result, tick)
        if tick == 1:
            normed, late = lax.optimization_barrier((normed, head_weight))
            (head_w,) = resident([[[late]]], 24)
            result, _, head_w = section_tick(state, normed, tick, beside=head_w)
            continue
        if tick < ticks - 1:
            result, _, _ = section_tick(state, normed, tick)
            continue
        done, normed = lax.optimization_barrier((result, normed))
        spread = spread_of(done, 0)
        result, blocks, _ = section_tick(
            state, normed, tick, beside=spread, after=lambda s: gathered(s)
        )
        with jax.named_scope("head0"):
            full = jnp.concatenate(blocks, axis=0)
            first = (full, core_swap(full))
    spread = spread_of(result, 1)
    spread, first = lax.optimization_barrier((spread, first))
    heads.append(head_block(where, *first, head_w, ids[0]))
    with jax.named_scope("head1"):
        blocks = gathered(spread)
        blocks, heads = lax.optimization_barrier((blocks, heads))
        full = jnp.concatenate(blocks, axis=0)
        heads.append(head_block(where, full, core_swap(full), head_w, ids[1]))

    with jax.named_scope("scores"):
        stats = jnp.concatenate([h[1] for h in heads], axis=1)[:3]
        stats = sent_to_all(stats, ("pipe", "tensor"))
        peak = jnp.max(stats[:, 0], axis=0)
        exp_total = jnp.sum(stats[:, 1] * jnp.exp(stats[:, 0] - peak), axis=0)
        target = jnp.sum(stats[:, 2], axis=0)
        log_norm = peak + jnp.log(exp_total)
        parts = score_block(
            [h[0] for h in heads], log_norm[None], ids, [h[2] for h in heads]
        )
        totals = sent_to_all(parts[:1, :micro], ("pipe", "tensor")).sum(axis=(0, 1))
        scores = jnp.sqrt(totals) / seq_len
        losses = (log_norm - target).reshape(micro, seq_len)
        token_loss = lax.dynamic_slice(
            losses, (0, loss_at), (micro, loss_width), allow_negative_indices=False
        )
    return (token_loss, scores)


def solution(mesh):
    in_specs = (
        P("dp", "tensor", None),
        P("dp", None),
        P("pipe", None),
        P("pipe", None, "tensor"),
        P("pipe", None, "tensor"),
        P("pipe", None, "tensor"),
        P("pipe", "tensor", None),
        P(),
        P(None, ("pipe", "tensor")),
    )
    out_specs = (P("dp", ("pipe", "tensor")), P("dp"))
    return jax.shard_map(
        per_device, mesh=mesh, in_specs=in_specs, out_specs=out_specs, check_vma=False
    )
```

```python
import functools
import math

import jax
import jax.numpy as jnp
from jax import lax
from jax.experimental import pallas as pl
from jax.experimental.pallas import tpu as pltpu
from jax.sharding import PartitionSpec as P

HD = 128
EPSILON = 1e-05
ROPE_BASE = 500000.0
CORES = 2
MIB = 1024 * 1024
F32, BF16 = jnp.float32, jnp.bfloat16
IN_VMEM = pl.BlockSpec(memory_space=pltpu.VMEM)
IN_SMEM = pl.BlockSpec(memory_space=pltpu.SMEM)
IN_HBM = pl.BlockSpec(memory_space=pltpu.HBM)


def sent_to_all(value, axis):
    size = lax.axis_size(axis)
    return lax.all_to_all(
        jnp.broadcast_to(value[None], (size, *value.shape)), axis, 0, 0, tiled=True
    )


def core_swap(value):
    size = lax.axis_size("tensor")
    return lax.ppermute(value, "tensor", [(t, t ^ 1) for t in range(size)])


def chip_swap(value, k):
    size = lax.axis_size("tensor")
    return lax.ppermute(value, "tensor", [(t, t ^ (CORES * k)) for t in range(size)])


def hop(value):
    size = lax.axis_size("pipe")
    return lax.ppermute(value, "pipe", [(i, i + 1) for i in range(size - 1)])


def normalize(states, gain_vec):
    values = states.astype(F32)
    return (
        values * lax.rsqrt(jnp.mean(values * values, axis=-1, keepdims=True) + EPSILON) * gain_vec
    )


def loader_kernel(*refs, plan):
    n_in = len(plan)
    ins, outs, sems = refs[:n_in], refs[n_in:-1], refs[-1]
    copies = []
    for i, (out, side, at) in enumerate(plan):
        target = outs[out].at[side, :, at : at + ins[i].shape[1]]
        copies.append(pltpu.make_async_copy(ins[i], target, sems.at[i]))
    for c in copies:
        c.start()
    for c in copies:
        c.wait()


def resident(arrays, room):
    flat = [w for sides in arrays for parts in sides for w in parts]
    plan, shapes = [], []
    for out, sides in enumerate(arrays):
        for side, parts in enumerate(sides):
            at = 0
            for w in parts:
                plan.append((out, side, at))
                at += w.shape[1]
        shapes.append(pltpu.VMEM((len(sides), sides[0][0].shape[0], at), BF16))
    return pl.pallas_call(
        functools.partial(loader_kernel, plan=plan),
        out_shape=shapes,
        in_specs=[IN_HBM] * len(flat),
        out_specs=[IN_VMEM] * len(shapes),
        scratch_shapes=[pltpu.SemaphoreType.DMA((len(flat),))],
        cost_estimate=pl.CostEstimate(
            flops=10**9, bytes_accessed=4 * sum(w.size for w in flat), transcendentals=0
        ),
        compiler_params=pltpu.CompilerParams(vmem_limit_bytes=room * MIB),
        name="resident",
    )(*flat)


def section_body(rows, context, state, w_in, w_out, cos_ref, sin_ref, bias_ref, outs, unrolled=False):
    cosine, sine, bias = cos_ref[...], sin_ref[...], bias_ref[...]
    n_rows = rows.shape[0]
    sides, depth, _ = w_out.shape

    def rotated(t):
        return (t * cosine + pltpu.roll(t, HD // 2, 1) * sine).astype(BF16)

    def attend(side, carry):
        both = jnp.dot(rows[...], w_in[side], preferred_element_type=F32)
        heads = both.shape[1] // HD - 2
        keys = rotated(both[:, heads * HD : (heads + 1) * HD])
        values = both[:, (heads + 1) * HD :].astype(BF16)
        stacked = jnp.concatenate(
            [rotated(both[:, h * HD : (h + 1) * HD]) for h in range(heads)], axis=0
        )
        logits = lax.dot_general(
            stacked, keys, (((1,), (1,)), ((), ())), preferred_element_type=F32
        ) / math.sqrt(HD)
        logits = logits + bias
        weights = jnp.exp(logits - jnp.max(logits, axis=-1, keepdims=True))
        probs = (weights / jnp.sum(weights, axis=-1, keepdims=True)).astype(BF16)
        out = jnp.dot(probs, values, preferred_element_type=F32).astype(BF16)
        context[side] = jnp.concatenate(
            [out[h * n_rows : (h + 1) * n_rows] for h in range(heads)], axis=1
        )
        return carry

    lax.fori_loop(0, sides, attend, 0)
    block, width = outs[0].shape
    step = width // 2

    def columns(cols):
        part = sum(
            jnp.dot(context[i], w_out[i, :, cols], preferred_element_type=F32)
            for i in range(sides)
        )
        outs[0][:, cols] = part[:block] + state[:, cols].astype(F32)
        for i in range(1, len(outs)):
            outs[i][:, cols] = part[i * block : (i + 1) * block].astype(BF16)

    if unrolled:
        for n in range(0, width, 512):
            columns(slice(n, n + 512))
        return

    def looped(c, carry):
        columns(pl.ds(pl.multiple_of(c * step, step), step))
        return carry

    lax.fori_loop(0, width // step, looped, 0)


def section_kernel(r0, r1, r2, r3, state, *rest):
    *rest, rows, context = rest
    block = r0.shape[0]
    for i, r in enumerate((r0, r1, r2, r3)):
        rows[i * block : (i + 1) * block, :] = r[...]
    section_body(rows, context, state, *rest[:5], rest[5:], unrolled=True)


def first_kernel(at_ref, whole, gain_ref, *rest):
    *rest, rows, context, state = rest
    chips = 4
    block = whole.shape[0] // chips
    for k in range(chips):
        row = jnp.bitwise_xor(at_ref[0], k) * block
        values = whole[pl.ds(pl.multiple_of(row, block), block), :]
        if k == 0:
            state[...] = values
        values = values.astype(F32)
        mean = jnp.mean(values * values, axis=-1, keepdims=True)
        normed = values * lax.rsqrt(mean + EPSILON) * gain_ref[...]
        rows[k * block : (k + 1) * block, :] = normed.astype(BF16)
    section_body(rows, context, state, *rest[:5], rest[5:])


def section_block(kernel, specs, entering, block, width, held, tables, scratch=()):
    shapes = [jax.ShapeDtypeStruct((block, width), F32)] + [
        jax.ShapeDtypeStruct((block, width), BF16)
    ] * 3
    n_rows = tables[0].shape[0]
    sides, depth, _ = held[1].shape
    return pl.pallas_call(
        kernel,
        out_shape=shapes,
        in_specs=specs + [IN_VMEM] * 5,
        out_specs=[IN_VMEM] * 4,
        scratch_shapes=[
            pltpu.VMEM((n_rows, width), BF16),
            pltpu.VMEM((sides, n_rows, depth), BF16),
            *scratch,
        ],
        cost_estimate=pl.CostEstimate(
            flops=8 * 10**9, bytes_accessed=2 * width * 1536, transcendentals=0
        ),
        compiler_params=pltpu.CompilerParams(vmem_limit_bytes=16 * MIB),
        name="section_block",
    )(*entering, *held, *tables)


def as_column(row):
    n = row.shape[1]
    return jnp.transpose(jnp.broadcast_to(row, (n, n)))[:, :1]


def head_kernel(
    at_ref, mine, theirs, w_ref, ids_ref, logits_ref, stats_ref, gram_ref, hidden
):
    chip, core = at_ref[0], at_ref[1]
    chips = 4
    block = mine.shape[0] // chips
    for side, rows in ((core, mine), (1 - core, theirs)):
        for k in range(chips):
            row = (side * chips + jnp.bitwise_xor(chip, k)) * block
            target = pl.ds(pl.multiple_of(row, block), block)
            hidden[target, :] = rows[k * block : (k + 1) * block, :]
    step = 256

    def columns(c, carry):
        cols = pl.ds(pl.multiple_of(c * step, step), step)
        logits_ref[:, cols] = jnp.dot(hidden[...], w_ref[0, :, cols], preferred_element_type=F32)
        return carry

    lax.fori_loop(0, w_ref.shape[2] // step, columns, 0)
    logits = logits_ref[...]
    n_rows, vocab = logits.shape
    hit = as_column(ids_ref[...]) == lax.broadcasted_iota(jnp.int32, (n_rows, vocab), 1).astype(F32)
    target = jnp.sum(jnp.where(hit, logits, 0.0), axis=1, keepdims=True)
    peak = jnp.max(logits, axis=1, keepdims=True)
    total = jnp.sum(jnp.exp(logits - peak), axis=1, keepdims=True)
    lane = lax.broadcasted_iota(jnp.int32, (n_rows, n_rows), 1)
    table = jnp.where(lane == 0, peak, jnp.where(lane == 1, total, target))
    stats_ref[...] = jnp.transpose(table)[:8]
    seq = n_rows // CORES
    for i in range(CORES):
        h = hidden[i * seq : (i + 1) * seq, :]
        gram_ref[i] = lax.dot_general(h, h, (((1,), (1,)), ((), ())), preferred_element_type=F32)


def head_block(where, mine, theirs, head_weight, ids):
    seq, width = mine.shape
    n_rows, vocab = CORES * seq, head_weight.shape[2]
    return pl.pallas_call(
        head_kernel,
        out_shape=[
            jax.ShapeDtypeStruct((n_rows, vocab), F32),
            jax.ShapeDtypeStruct((8, n_rows), F32),
            jax.ShapeDtypeStruct((CORES, seq, seq), F32),
        ],
        in_specs=[IN_SMEM] + [IN_VMEM] * 4,
        out_specs=[IN_VMEM] * 3,
        scratch_shapes=[pltpu.VMEM((n_rows, width), BF16)],
        cost_estimate=pl.CostEstimate(
            flops=4 * 10**9, bytes_accessed=2 * width * vocab, transcendentals=0
        ),
        compiler_params=pltpu.CompilerParams(vmem_limit_bytes=16 * MIB),
        name="head_block",
    )(where, mine, theirs, head_weight, ids)


def score_kernel(l0, l1, norm_ref, i0, i1, g0, g1, out_ref):
    chain_rows, vocab = l0.shape
    seq = chain_rows // CORES
    lane = lax.broadcasted_iota(jnp.int32, (8, 128), 1)
    result = jnp.zeros((8, 128), F32)
    for j, (logits, ids, gram) in enumerate(((l0, i0, g0), (l1, i1, g1))):
        norm = as_column(norm_ref[:, j * chain_rows : (j + 1) * chain_rows])
        entry = lax.broadcasted_iota(jnp.int32, (chain_rows, vocab), 1).astype(F32)
        hit = as_column(ids[...]) == entry
        errors = jnp.exp(logits[...] - norm) - hit.astype(F32)
        errors = errors.astype(BF16)
        for i in range(CORES):
            e = errors[i * seq : (i + 1) * seq]
            pair = lax.dot_general(e, e, (((1,), (1,)), ((), ())), preferred_element_type=F32)
            result = jnp.where(lane == j * CORES + i, jnp.sum(pair * gram[i]), result)
    out_ref[...] = result


def score_block(logits, log_norm, ids, grams):
    return pl.pallas_call(
        score_kernel,
        out_shape=jax.ShapeDtypeStruct((8, 128), F32),
        in_specs=[IN_VMEM] * 7,
        out_specs=IN_VMEM,
        cost_estimate=pl.CostEstimate(flops=10**9, bytes_accessed=10**6, transcendentals=0),
        compiler_params=pltpu.CompilerParams(vmem_limit_bytes=12 * MIB),
        name="score_block",
    )(*logits, log_norm, *ids, *grams)


def per_device(embeds, labels, norm_gain, w_query, w_key, w_value, w_out, final_gain, head_weight):
    pipe_count = lax.axis_size("pipe")
    tensor_count = lax.axis_size("tensor")
    chips = tensor_count // CORES
    section = lax.axis_index("pipe")
    rank = lax.axis_index("tensor")
    chip, core = rank // CORES, rank % CORES
    micro, own_rows, width = embeds.shape
    chains = micro // CORES
    seq_len = own_rows * tensor_count
    block = own_rows * CORES

    own_w = (w_query[0], w_key[0], w_value[0], w_out[0])
    vocab_dev = head_weight.shape[1]
    slot = section * tensor_count + rank
    loss_width = seq_len // (pipe_count * tensor_count)
    at_section = [section == p for p in range(pipe_count - 1)]
    scalars = (core == 0, at_section, slot * vocab_dev, slot * loss_width, chip, core)
    embeds, scalars = lax.optimization_barrier((embeds, scalars))
    on_first, at_section, first_id, loss_at, chip, core = scalars
    ids = (labels - first_id).astype(F32).reshape(chains, 1, CORES * seq_len)
    where = jnp.stack([chip, core]).astype(jnp.int32)

    first_rows = jnp.broadcast_to(embeds[:CORES][None], (chips, CORES, own_rows, width))
    first_rows = first_rows.reshape(tensor_count, own_rows, width)
    whole = lax.all_to_all(first_rows, "tensor", 0, 0, tiled=True).reshape(seq_len, width)
    other_w = [core_swap(w) for w in own_w]

    later = embeds[CORES:].reshape(chains - 1, CORES, own_rows, width)
    mine = jnp.where(on_first, later[:, 0], later[:, 1])
    got = core_swap(jnp.where(on_first, later[:, 1], later[:, 0]))
    start = jnp.where(
        on_first, jnp.concatenate([mine, got], axis=1), jnp.concatenate([got, mine], axis=1)
    )

    at = jnp.arange(seq_len, dtype=jnp.int32)
    place = jnp.bitwise_xor(chip, at // block) * block + at % block
    half = HD // 2
    inverse = ROPE_BASE ** (-2.0 * jnp.arange(half, dtype=F32) / HD)
    angles = place.astype(F32)[:, None] * inverse[None, :]
    cosine, sine = jnp.cos(angles), jnp.sin(angles)
    cosine = jnp.concatenate([cosine, cosine], axis=1)
    sine = jnp.concatenate([-sine, sine], axis=1)
    bias = jnp.where(place[:, None] >= place[None, :], 0.0, -1e30)
    bias = jnp.concatenate([bias] * (own_w[0].shape[1] // HD), axis=0)

    def gathered(rows):
        return [rows] + [chip_swap(rows, k) for k in range(1, chips)]

    tables = (cosine, sine, bias)
    ready = lax.optimization_barrier((whole, [*ids], where, tables, own_w))
    whole, ids, where, tables, own_w = ready
    held = resident(
        [[own_w[:3], other_w[:3]], [own_w[3:], other_w[3:]]],
        48,
    )

    def summed(parts, after=()):
        got = [chip_swap(parts[k], k) for k in range(1, chips)]
        got, after = lax.optimization_barrier((got, after))
        total = parts[0]
        for g in got:
            total = total + g.astype(F32)
        return total.astype(BF16), after

    def section_tick(state, normed, tick, beside=(), after=()):
        with jax.named_scope(f"tick{tick}"):
            blocks = gathered(normed)
            blocks, beside = lax.optimization_barrier((blocks, beside))
            after = after(beside) if after else ()
            parts = section_block(
                section_kernel,
                [IN_VMEM] * 5,
                (*blocks, state),
                block,
                width,
                held,
                tables,
            )
            return (*summed(parts, after), beside)

    def next_state(result, tick):
        with jax.named_scope(f"hop{tick}"):
            state = hop(result)
            if tick < chains:
                state = jnp.where(at_section[0], start[tick - 1], state)
            return state, normalize(state, norm_gain[0]).astype(BF16)

    def spread_of(result, j):
        with jax.named_scope(f"spread{j}"):
            hidden = normalize(result, final_gain).astype(BF16)
            here = [
                lax.ppermute(hidden, "pipe", [(pipe_count - 1, p)]) for p in range(pipe_count - 1)
            ]
            spread = hidden
            for p in range(pipe_count - 1):
                spread = jnp.where(at_section[p], here[p], spread)
            return spread

    with jax.named_scope("tick0"):
        parts = section_block(
            first_kernel,
            [IN_SMEM, IN_VMEM, IN_VMEM],
            (where, whole, norm_gain),
            block,
            width,
            held,
            tables,
            scratch=[pltpu.VMEM((block, width), BF16)],
        )
        result, _ = summed(parts)
    ticks = chains + pipe_count - 1
    heads = []
    for tick in range(1, ticks):
        state, normed = next_state(result, tick)
        if tick == 1:
            normed, late = lax.optimization_barrier((normed, head_weight))
            (head_w,) = resident([[[late]]], 24)
            result, _, head_w = section_tick(state, normed, tick, beside=head_w)
            continue
        if tick < ticks - 1:
            result, _, _ = section_tick(state, normed, tick)
            continue
        done, normed = lax.optimization_barrier((result, normed))
        spread = spread_of(done, 0)
        result, blocks, _ = section_tick(
            state, normed, tick, beside=spread, after=lambda s: gathered(s)
        )
        with jax.named_scope("head0"):
            full = jnp.concatenate(blocks, axis=0)
            first = (full, core_swap(full))
    spread = spread_of(result, 1)
    spread, first = lax.optimization_barrier((spread, first))
    heads.append(head_block(where, *first, head_w, ids[0]))
    with jax.named_scope("head1"):
        blocks = gathered(spread)
        blocks, heads = lax.optimization_barrier((blocks, heads))
        full = jnp.concatenate(blocks, axis=0)
        heads.append(head_block(where, full, core_swap(full), head_w, ids[1]))

    with jax.named_scope("scores"):
        stats = jnp.concatenate([h[1] for h in heads], axis=1)[:3]
        stats = sent_to_all(stats, ("pipe", "tensor"))
        peak = jnp.max(stats[:, 0], axis=0)
        exp_total = jnp.sum(stats[:, 1] * jnp.exp(stats[:, 0] - peak), axis=0)
        target = jnp.sum(stats[:, 2], axis=0)
        log_norm = peak + jnp.log(exp_total)
        parts = score_block(
            [h[0] for h in heads], log_norm[None], ids, [h[2] for h in heads]
        )
        totals = sent_to_all(parts[:1, :micro], ("pipe", "tensor")).sum(axis=(0, 1))
        scores = jnp.sqrt(totals) / seq_len
        losses = (log_norm - target).reshape(micro, seq_len)
        token_loss = lax.dynamic_slice(
            losses, (0, loss_at), (micro, loss_width), allow_negative_indices=False
        )
    return (token_loss, scores)


def solution(mesh):
    in_specs = (
        P("dp", "tensor", None),
        P("dp", None),
        P("pipe", None),
        P("pipe", None, "tensor"),
        P("pipe", None, "tensor"),
        P("pipe", None, "tensor"),
        P("pipe", "tensor", None),
        P(),
        P(None, ("pipe", "tensor")),
    )
    out_specs = (P("dp", ("pipe", "tensor")), P("dp"))
    return jax.shard_map(
        per_device, mesh=mesh, in_specs=in_specs, out_specs=out_specs, check_vma=False
    )
```
